16 devices in a mesh: data: 2 (over y, z), model: 8 (over x, core).
Axes of the slice: x: 4, y: 2, z: 1, core: 2. Of those that a mesh axis runs over, the one named last changes fastest.
The devices are a block of a 4x4x8 slice.
Arguments:
- queries: bfloat16 [512, 1024], P('data'), parts along dimension 0
- w_head: bfloat16 [1024, 50304], P(None, 'model')
- ds_keys: bfloat16 [524288, 1024], P('model')
- ds_tokens: int32 [524288], P('model')
- temperature: float32 [1], replicated
- mix_weight: float32 [1], replicated
Outputs:
- output: float32 [512, 50304], P('data', 'model'), parts along dimension 0
There are 2 independent parts. The reference program is written for one: setup_inputs(seed, part) draws one part's arguments, and reference() takes and returns one part's arrays. A program takes and returns all parts, laid end to end along the dimension named above; an argument that names none is the same for every part.
All inputs are finite; a program needn't handle non-finite values.
Results may differ from the reference program's by a relative error of at most 0.001.
Values are sent between devices in bfloat16 or wider.
A program may use at most 768 MiB of HBM per device.

```python
import jax
import jax.numpy as jnp
from jax import lax

Q_ROWS = 256
D_MODEL = 1024
VOCAB_SIZE = 50304
N_LOCAL = 65536
GROUP_SIZE = 8


def setup_inputs(seed: int = 0, part: int = 0) -> dict:
    root_key = jax.random.key(seed)
    key_query, key_head, key_store, key_token, key_temp, key_mix = jax.random.split(root_key, 6)
    key_query = jax.random.fold_in(key_query, part)
    n_total = GROUP_SIZE * N_LOCAL
    queries = jax.random.normal(key_query, (Q_ROWS, D_MODEL), jnp.float32)
    w_head = jax.random.normal(key_head, (D_MODEL, VOCAB_SIZE), jnp.float32) * (2.0 * D_MODEL ** -0.5)
    ds_keys = jax.random.normal(key_store, (n_total, D_MODEL), jnp.float32)
    ds_tokens = jax.random.randint(key_token, (n_total,), 0, VOCAB_SIZE, jnp.int32)
    ds_tokens = ds_tokens.at[0].set(VOCAB_SIZE - 1).at[1].set(0)
    temperature = jax.random.uniform(key_temp, (1,), jnp.float32, 0.7, 0.95) * (D_MODEL ** 0.5)
    mix_weight = jax.random.uniform(key_mix, (1,), jnp.float32, 0.25, 0.5)
    return {
        "queries": queries.astype(jnp.bfloat16),
        "w_head": w_head.astype(jnp.bfloat16),
        "ds_keys": ds_keys.astype(jnp.bfloat16),
        "ds_tokens": ds_tokens,
        "temperature": temperature,
        "mix_weight": mix_weight,
    }


def reference(queries, w_head, ds_keys, ds_tokens, temperature, mix_weight):
    key_blocks = ds_keys.reshape(GROUP_SIZE, N_LOCAL, D_MODEL)
    tok_blocks = ds_tokens.reshape(GROUP_SIZE, N_LOCAL)
    temp_value = temperature[0]

    def block_scores(key_block):
        cross_dot = jnp.dot(queries, key_block.T, preferred_element_type=jnp.float32)
        key_sq = jnp.sum(jnp.square(key_block.astype(jnp.float32)), axis=1)
        return (2.0 * cross_dot - key_sq[None, :]) / temp_value

    block_max = lax.map(lambda key_block: jnp.max(block_scores(key_block), axis=1), key_blocks)
    row_max = jnp.max(block_max, axis=0)

    def accumulate(carry_state, block_pair):
        histogram, row_total = carry_state
        key_block, tok_block = block_pair
        weights = jnp.exp(block_scores(key_block) - row_max[:, None])
        histogram = histogram.at[:, tok_block].add(weights)
        return (histogram, row_total + jnp.sum(weights, axis=1)), None

    start_state = (jnp.zeros((Q_ROWS, VOCAB_SIZE), jnp.float32), jnp.zeros((Q_ROWS,), jnp.float32))
    (histogram, row_total), unused = lax.scan(accumulate, start_state, (key_blocks, tok_blocks))
    logits = jnp.dot(queries, w_head, preferred_element_type=jnp.float32)
    lm_exp = jnp.exp(logits - jnp.max(logits, axis=1, keepdims=True))
    p_lm = lm_exp / jnp.sum(lm_exp, axis=1, keepdims=True)
    mix_value = mix_weight[0]
    return jnp.log(mix_value * histogram / row_total[:, None] + (1.0 - mix_value) * p_lm)
```

```python
import functools

import jax
import jax.numpy as jnp
from jax import lax
from jax.experimental import pallas as pl
from jax.experimental.pallas import tpu as pltpu
from jax.sharding import PartitionSpec as P

BLOCK = 1024
UNROLL = 16
GROUPS = 4
SLOTS = 3
SLACK = 40.0


def hist_kernel(inv_tau_ref, flag_ref, tok_ref, keys_ref, qt_ref, out_ref, stat_ref,
                hist, w, sbuf, held, m_ref, z_ref, sems, key_sem):
    i = pl.program_id(0)
    blk = held.shape[1]
    blocks = pl.num_programs(0)

    def fetch(b):
        return pltpu.make_async_copy(keys_ref.at[pl.ds(b * blk, blk), :], held.at[b % SLOTS], key_sem.at[b % SLOTS])

    @pl.when(i == 0)
    def _():
        for b in range(SLOTS - 1):
            fetch(b).start()

    @pl.when(i + SLOTS - 1 < blocks)
    def _():
        fetch(i + SLOTS - 1).start()
    fetch(i).wait()
    key_ref = held.at[i % SLOTS]
    stride = blk // UNROLL
    total = hist.shape[0]
    H = lambda t: pl.ds(pl.multiple_of(t, 2), 2)
    W = lambda e: pl.ds(pl.multiple_of(2 * e, 2), 2)

    inv_tau = inv_tau_ref[0]
    qt = qt_ref[...]
    mb = None
    for r in range(0, blk, 256):
        k = key_ref[pl.ds(r, 256), :]
        c = jnp.dot(k, qt, preferred_element_type=jnp.float32)
        kf = k.astype(jnp.float32)
        sq = jnp.sum(kf * kf, axis=1, keepdims=True)
        s = (2.0 * c - sq) * inv_tau
        sbuf[pl.ds(r, 256), :] = s
        mx = jnp.max(s, axis=0, keepdims=True)
        mb = mx if mb is None else jnp.maximum(mb, mx)
    mb2 = jnp.concatenate([mb[:, :128], mb[:, 128:]], axis=0)

    @pl.when(i == 0)
    def _():
        m_ref[...] = mb2
        z_ref[...] = jnp.zeros_like(z_ref)

        def zero(t, c):
            hist[pl.ds(pl.multiple_of(t * 96, 96), 96), :] = jnp.zeros((96, 128), jnp.float32)
            return c
        lax.fori_loop(0, total // 96, zero, 0)

    @pl.when(jnp.max(mb2 - m_ref[...]) > SLACK)
    def _():
        new = jnp.maximum(m_ref[...], mb2)
        f = jnp.exp(m_ref[...] - new)
        m_ref[...] = new
        z_ref[...] = z_ref[...] * f
        f96 = jnp.concatenate([f] * 48, axis=0)

        def scale(t, c):
            sl = pl.ds(pl.multiple_of(t * 96, 96), 96)
            hist[sl, :] = hist[sl, :] * f96
            return c
        lax.fori_loop(0, total // 96, scale, 0)

    m = m_ref[...]
    mrow = jnp.concatenate([m[0:1], m[1:2]], axis=1)

    def expo(t, acc):
        e = jnp.exp(sbuf[pl.ds(pl.multiple_of(t * 64, 64), 64), :] - mrow)
        w[pl.ds(pl.multiple_of(t * 128, 128), 64, stride=2), :] = e[:, :128]
        w[pl.ds(pl.multiple_of(t * 128, 128) + 1, 64, stride=2), :] = e[:, 128:]
        return acc + jnp.sum(e.reshape(8, 8, 256), axis=0)
    za = lax.fori_loop(0, blk // 64, expo, jnp.zeros((8, 256), jnp.float32))
    za = jnp.sum(za, axis=0, keepdims=True)
    z_ref[...] = z_ref[...] + jnp.concatenate([za[:, :128], za[:, 128:]], axis=0)

    def step(g, c):
        def fast():
            for gg in range(GROUPS):
                at = [g * GROUPS + gg + u * stride for u in range(UNROLL)]
                ts = [tok_ref[0, 0, a] for a in at]
                vs = [hist[H(t), :] + w[W(a), :] for t, a in zip(ts, at)]
                for t, v in zip(ts, vs):
                    hist[H(t), :] = v

        def slow():
            def one(e, c):
                a = g * GROUPS + e // UNROLL + (e % UNROLL) * stride
                t = tok_ref[0, 0, a]
                hist[H(t), :] = hist[H(t), :] + w[W(a), :]
                return c
            lax.fori_loop(0, GROUPS * UNROLL, one, 0)
        lax.cond(flag_ref[0, 0, g] == 0, fast, slow)
        return c
    lax.fori_loop(0, stride // GROUPS, step, 0)

    @pl.when(i == pl.num_programs(0) - 1)
    def _():
        stat_ref[0:2, :] = m_ref[...]
        stat_ref[2:4, :] = z_ref[...]
        stat_ref[4:8, :] = jnp.zeros((4, 128), jnp.float32)
        part = total // 8
        copies = [pltpu.make_async_copy(hist.at[pl.ds(p * part, part), :], out_ref.at[pl.ds(p * part, part), :], sems.at[p])
                  for p in range(8)]
        for copy in copies:
            copy.start()
        for copy in copies:
            copy.wait()


def histogram(keys, qt, tok, inv_tau, vocab):
    count, depth = keys.shape
    blocks = count // BLOCK
    stride = BLOCK // UNROLL
    members = tok.reshape(blocks, UNROLL, stride)
    clash = jnp.zeros((blocks, stride), jnp.bool_)
    for d in range(1, UNROLL):
        clash = clash | jnp.any(members[:, d:] == members[:, :-d], axis=1)
    flags = jnp.any(clash.reshape(blocks, 1, stride // GROUPS, GROUPS), axis=3).astype(jnp.int32)
    f32 = jnp.float32
    return pl.pallas_call(
        hist_kernel,
        grid=(blocks,),
        out_shape=(jax.ShapeDtypeStruct((2 * vocab, 128), f32), jax.ShapeDtypeStruct((8, 128), f32)),
        in_specs=[
            pl.BlockSpec(memory_space=pltpu.SMEM),
            pl.BlockSpec((1, 1, stride // GROUPS), lambda i: (i, 0, 0), memory_space=pltpu.SMEM),
            pl.BlockSpec((1, 1, BLOCK), lambda i: (i, 0, 0), memory_space=pltpu.SMEM),
            pl.BlockSpec(memory_space=pl.ANY),
            pl.BlockSpec((depth, qt.shape[1]), lambda i: (0, 0)),
        ],
        out_specs=(pl.BlockSpec(memory_space=pl.ANY), pl.BlockSpec((8, 128), lambda i: (0, 0))),
        scratch_shapes=[
            pltpu.VMEM((2 * vocab, 128), f32),
            pltpu.VMEM((2 * BLOCK, 128), f32),
            pltpu.VMEM((BLOCK, qt.shape[1]), f32),
            pltpu.VMEM((SLOTS, BLOCK, depth), keys.dtype),
            pltpu.VMEM((2, 128), f32),
            pltpu.VMEM((2, 128), f32),
            pltpu.SemaphoreType.DMA((8,)),
            pltpu.SemaphoreType.DMA((SLOTS,)),
        ],
        compiler_params=pltpu.CompilerParams(vmem_limit_bytes=67043328, dimension_semantics=("arbitrary",)),
        name="histogram",
    )(inv_tau, flags, (2 * tok).reshape(blocks, 1, BLOCK), keys, qt)


def exchange_kernel(group, mix_ref, stat_ref, qt_ref, hist_ref, wt_ref, out_ref,
                    sib, fwd, fin, own, lm, wtile, obuf, stats, lmstat, lmstats,
                    sib_send, sib_recv, fwd_send, fwd_recv, fin_send, fin_recv,
                    st_send, st_recv, ls_send, ls_recv, own_sem, w_sem, o_sem):
    chips = group // 2
    me = lax.axis_index("model")
    x, core = me // 2, me % 2
    sibling = 2 * x + 1 - core
    right = 2 * ((x + 1) % chips) + core
    left = 2 * ((x + chips - 1) % chips) + core
    side = (right, left)
    subs = fwd.shape[1]
    rows = fwd.shape[2]
    toks = rows // 2
    half_rows = subs * rows
    block_rows = 2 * half_rows
    where = lambda d: dict(device_id={"model": d}, device_id_type=pl.DeviceIdType.MESH)

    def place(stage, s, d, c):
        chip = {0: (x + 2) % chips, 1: (x + (1, chips - 1)[d]) % chips, 2: (x + (1, chips - 1)[d]) % chips, 3: x}[stage]
        half = 1 - d if stage == 1 else d
        return pl.ds(pl.multiple_of((2 * chip + c) * block_rows + half * half_rows + s * rows, 8), rows)

    def order(stage, s, d):
        return (stage * subs + s) * 2 + d

    def to_sibling(stage, s, d):
        k = order(stage, s, d)
        return pltpu.make_async_remote_copy(hist_ref.at[place(stage, s, d, 1 - core), :], sib.at[k],
                                            sib_send.at[k], sib_recv.at[k], **where(sibling))

    def own_copy(stage, s, d):
        return pltpu.make_async_copy(hist_ref.at[place(stage, s, d, core), :], own.at[d], own_sem.at[d])

    def hop(d, s):
        return pltpu.make_async_remote_copy(sib.at[order(0, s, d)], fwd.at[d, s], fwd_send.at[d, s], fwd_recv.at[d, s], **where(side[d]))

    def last(d, stage, s):
        k = (stage - 1) * subs + s
        return pltpu.make_async_remote_copy(sib.at[order(stage, s, d)], fin.at[d, k], fin_send.at[d, k], fin_recv.at[d, k], **where(side[d]))

    barrier = pltpu.get_barrier_semaphore()
    for j in range(1, group):
        pl.semaphore_signal(barrier, inc=1, **where((me + j) % group))
    pl.semaphore_wait(barrier, group - 1)

    def stat_copy(j):
        return pltpu.make_async_remote_copy(stat_ref, stats.at[me], st_send.at[j], st_recv.at[j], **where((me + j) % group))

    for j in range(1, group):
        stat_copy(j).start()
    for stage in range(4):
        def issue(s, c, stage=stage):
            for d in range(2):
                to_sibling(stage, s, d).start()
            return c
        lax.fori_loop(0, subs, issue, 0)
    own_copy(0, 0, 0).start()
    own_copy(0, 0, 1).start()
    stats[me] = stat_ref[...]
    tiles = lm.shape[0] // toks

    def w_copy(t):
        return pltpu.make_async_copy(wt_ref.at[pl.ds(t * toks, toks), :], wtile, w_sem)
    w_copy(0).start()
    for j in range(1, group):
        stat_copy(j).wait()

    ms = [stats[i, 0:2, :] for i in range(group)]
    top = functools.reduce(jnp.maximum, ms)
    total = functools.reduce(jnp.add, [stats[i, 2:4, :] * jnp.exp(ms[i] - top) for i in range(group)])
    tile8 = lambda v: jnp.concatenate([v] * 4, axis=0)[None]
    mine = tile8(jnp.exp(stats[me, 0:2, :] - top))
    other = tile8(jnp.exp(stats[sibling, 0:2, :] - top))
    fold = lambda v: v.reshape(rows // 8, 8, 128)

    def merge(stage, s, d):
        k = order(stage, s, d)
        own_copy(stage, s, d).wait()
        to_sibling(stage, s, d).wait_recv()
        return fold(own[d]) * mine + fold(sib[k]) * other

    def prefetch(stage, s, d):
        @pl.when(s + 1 < subs)
        def _():
            own_copy(stage, s + 1, d).start()
        if stage < 3:
            @pl.when(s + 1 == subs)
            def _():
                own_copy(stage + 1, 0, d).start()

    def stage0(s, c):
        for d in range(2):
            v = merge(0, s, d)
            sib[order(0, s, d)] = v.reshape(rows, 128)
            hop(d, s).start()
            prefetch(0, s, d)
        return c
    lax.fori_loop(0, subs, stage0, 0)

    def stage1(s, c):
        for d in range(2):
            v = merge(1, s, d)
            sib[order(1, s, d)] = v.reshape(rows, 128)
            last(d, 1, s).start()
            prefetch(1, s, d)
        return c
    lax.fori_loop(0, subs, stage1, 0)

    qt = qt_ref[...]
    peak = None
    for t in range(tiles):
        w_copy(t).wait()
        logits = jnp.dot(wtile[...], qt, preferred_element_type=jnp.float32)
        lm[pl.ds(t * toks, toks), :] = logits
        if t + 1 < tiles:
            w_copy(t + 1).start()
        mx = jnp.max(logits.reshape(toks // 8, 8, 256), axis=0)
        peak = mx if peak is None else jnp.maximum(peak, mx)
    peak = jnp.max(peak, axis=0, keepdims=True)

    def expo(t, acc):
        sl = pl.ds(pl.multiple_of(t * 48, 48), 48)
        e = jnp.exp(lm[sl, :] - peak)
        lm[sl, :] = e
        return acc + jnp.sum(e.reshape(6, 8, 256), axis=0)
    acc = lax.fori_loop(0, lm.shape[0] // 48, expo, jnp.zeros((8, 256), jnp.float32))
    acc = jnp.sum(acc, axis=0, keepdims=True)
    lmstat[0:1, :] = peak
    lmstat[1:2, :] = acc
    lmstat[2:8, :] = jnp.zeros((6, 256), jnp.float32)
    lmstats[me, 0:1, :] = peak
    lmstats[me, 1:2, :] = acc

    def ls_copy(j):
        return pltpu.make_async_remote_copy(lmstat, lmstats.at[me], ls_send.at[j], ls_recv.at[j], **where((me + j) % group))

    def stage2(s, c):
        for d in range(2):
            v = merge(2, s, d)
            hop(d, s).wait_recv()
            sib[order(2, s, d)] = (v + fold(fwd[d, s])).reshape(rows, 128)
            last(d, 2, s).start()
            prefetch(2, s, d)
        return c

    for j in range(1, group):
        ls_copy(j).start()
    lax.fori_loop(0, subs, stage2, 0)
    for j in range(1, group):
        ls_copy(j).wait()

    lms = [lmstats[i, 0:1, :] for i in range(group)]
    lm_top = functools.reduce(jnp.maximum, lms)
    lm_total = functools.reduce(jnp.add, [lmstats[i, 1:2, :] * jnp.exp(lms[i] - lm_top) for i in range(group)])
    mix = mix_ref[0]
    lm_scale = (1.0 - mix) * (jnp.exp(peak - lm_top) / lm_total)
    knn_scale = mix / total
    knn_row = jnp.concatenate([knn_scale[0:1], knn_scale[1:2]], axis=1)

    def out_copy(s, d):
        return pltpu.make_async_copy(obuf.at[d], out_ref.at[pl.ds(pl.multiple_of((d * subs + s) * toks, 8), toks), :], o_sem.at[d])

    def stage3(s, c):
        for d in range(2):
            k = order(3, s, d)
            v = merge(3, s, d)
            last(1 - d, 1, s).wait_recv()
            v = v + fold(fin[1 - d, s])
            last(d, 2, s).wait_recv()
            v = v + fold(fin[d, subs + s])
            sib[k] = v.reshape(rows, 128)
            prefetch(3, s, d)

            @pl.when(s > 0)
            def _():
                out_copy(s - 1, d).wait()
            hk = jnp.concatenate([sib[k, pl.ds(0, toks, stride=2), :], sib[k, pl.ds(1, toks, stride=2), :]], axis=1)
            e = lm[pl.ds(pl.multiple_of((d * subs + s) * toks, 8), toks), :]
            obuf[d] = hk * knn_row + e * lm_scale
            out_copy(s, d).start()
        return c
    lax.fori_loop(0, subs, stage3, 0)
    for d in range(2):
        out_copy(subs - 1, d).wait()

    def drain(s, c):
        for stage in range(4):
            for d in range(2):
                to_sibling(stage, s, d).wait_send()
        for d in range(2):
            hop(d, s).wait_send()
            last(d, 1, s).wait_send()
            last(d, 2, s).wait_send()
        return c
    lax.fori_loop(0, subs, drain, 0)


def exchange(hist, stat, qt, wt, mix, group):
    cols = wt.shape[0]
    subs = next(n for n in range(3, cols) if cols % (2 * n * 8) == 0)
    toks = cols // (2 * subs)
    rows = 2 * toks
    dma = pltpu.SemaphoreType.DMA
    f32 = jnp.float32
    return pl.pallas_call(
        functools.partial(exchange_kernel, group),
        out_shape=jax.ShapeDtypeStruct((cols, qt.shape[1]), f32),
        in_specs=[
            pl.BlockSpec(memory_space=pltpu.SMEM),
            pl.BlockSpec(memory_space=pltpu.VMEM),
            pl.BlockSpec(memory_space=pltpu.VMEM),
            pl.BlockSpec(memory_space=pl.ANY),
            pl.BlockSpec(memory_space=pl.ANY),
        ],
        out_specs=pl.BlockSpec(memory_space=pl.ANY),
        scratch_shapes=[
            pltpu.VMEM((8 * subs, rows, 128), f32),
            pltpu.VMEM((2, subs, rows, 128), f32),
            pltpu.VMEM((2, 2 * subs, rows, 128), f32),
            pltpu.VMEM((2, rows, 128), f32),
            pltpu.VMEM((cols, qt.shape[1]), f32),
            pltpu.VMEM((toks, wt.shape[1]), wt.dtype),
            pltpu.VMEM((2, toks, qt.shape[1]), f32),
            pltpu.VMEM((group, 8, 128), f32),
            pltpu.VMEM((8, qt.shape[1]), f32),
            pltpu.VMEM((group, 8, qt.shape[1]), f32),
            dma((8 * subs,)), dma((8 * subs,)),
            dma((2, subs)), dma((2, subs)),
            dma((2, 2 * subs)), dma((2, 2 * subs)),
            dma((group,)), dma((group,)), dma((group,)), dma((group,)),
            dma((2,)), dma, dma((2,)),
        ],
        compiler_params=pltpu.CompilerParams(collective_id=0, has_side_effects=True, vmem_limit_bytes=67043328),
        name="exchange",
    )(mix, stat, qt, hist, wt)


def solution(mesh):
    group = mesh.shape["model"]

    def local_step(queries, w_shard, key_shard, tok_shard, temperature, mix_weight):
        qt = queries.T
        vocab = w_shard.shape[1] * group
        hist, stat = histogram(key_shard, qt, tok_shard, 1.0 / temperature, vocab)
        mixed = exchange(hist, stat, qt, w_shard.T, mix_weight, group)
        return jnp.log(mixed).T

    return jax.shard_map(
        local_step,
        mesh=mesh,
        in_specs=(P("data", None), P(None, "model"), P("model", None), P("model"), P(), P()),
        out_specs=P("data", "model"),
        check_vma=False,
    )
```

```python
import functools

import jax
import jax.numpy as jnp
from jax import lax
from jax.experimental import pallas as pl
from jax.experimental.pallas import tpu as pltpu
from jax.sharding import PartitionSpec as P

CHUNK = 512
PIECE = 256
UNROLL = 4
SLOTS = 5
SLACK = 40.0
STEP = 32


def hist_kernel(inv_tau_ref, zero_ref, first_ref, next_ref, used_ref, rows_ref, keys_ref, qt_ref, out_ref, stat_ref,
                hist, w_a, w_b, held, t_a, t_b, t_c, t_d, all_ref, m_ref, peak_ref, part_ref, z_ref, sems, key_sem, tok_sem):
    size = held.shape[1]
    chunks = keys_ref.shape[0] // size
    stride = size // UNROLL
    total = out_ref.shape[0]
    zero = zero_ref[0]
    H = lambda t: pl.ds(pl.multiple_of(t, 2), 2)
    W = lambda e: pl.ds(pl.multiple_of(zero + 2 * e, 2), 2)
    twice = 2.0 * inv_tau_ref[0]

    def fetch(c):
        return pltpu.make_async_copy(keys_ref.at[pl.ds(c * size, size), :], held.at[c % SLOTS], key_sem.at[c % SLOTS])

    tokens = (t_a, t_b, t_c, t_d)
    turns = len(tokens)

    def tok_fetch(c, turn):
        return [pltpu.make_async_copy(used_ref.at[c], tokens[turn], tok_sem.at[turn, 0]),
                pltpu.make_async_copy(rows_ref.at[c], all_ref.at[turn], tok_sem.at[turn, 1])]

    def score(c, w, beside=()):
        slot = c % SLOTS
        qt = qt_ref[...]
        m8 = m_ref[...]
        peak, part = None, None
        for r in range(0, size, PIECE):
            cross = jnp.dot(held[slot, pl.ds(r, PIECE), :], qt, preferred_element_type=jnp.float32)
            for b in range(0, PIECE, STEP):
                kf = held[slot, pl.ds(r + b, STEP), :].astype(jnp.float32)
                half = 0.5 * jnp.sum(kf * kf, axis=1, keepdims=True)
                s = ((cross[b:b + STEP] - half) * twice).reshape(STEP // 8, 8, 256)
                e = jnp.exp(s - m8[None])
                mx, sm = jnp.max(s, axis=0), jnp.sum(e, axis=0)
                peak = mx if peak is None else jnp.maximum(peak, mx)
                part = sm if part is None else part + sm
                e = e.reshape(STEP, 256)
                w[pl.ds(2 * (r + b), STEP, stride=2), :] = e[:, :128]
                w[pl.ds(2 * (r + b) + 1, STEP, stride=2), :] = e[:, 128:]
        for add in beside:
            add()
        peak_ref[...] = peak
        part_ref[...] = part
        return jnp.max(peak - m8) > SLACK

    def spread(v):
        return jnp.broadcast_to(jnp.max(v, axis=0, keepdims=True), v.shape)

    def adds(turn, w):
        toks = tokens[turn]
        ahead = []

        def step(j):
            if j < stride:
                ts = [toks[0, j + u * stride] for u in range(UNROLL)]
                ahead.append([(t, hist[H(t), :] + w[W(j + u * stride), :]) for u, t in enumerate(ts)])
            if j > 0:
                for t, v in ahead.pop(0):
                    hist[H(t), :] = v
        return [functools.partial(step, j) for j in range(stride + 1)]

    def repeats(c, turn, w):
        def step(j):
            def one(u, carry):
                a = j + u * stride
                t = all_ref[turn, 0, a]

                @pl.when(tokens[turn][0, a] != t)
                def _():
                    hist[H(t), :] = hist[H(t), :] + w[W(a), :]
                return carry
            lax.fori_loop(0, UNROLL, one, 0)
            return next_ref[c * stride + j]
        lax.while_loop(lambda j: j < stride, step, first_ref[c])

    def advance(c, turn, cur, nxt):
        for copy in tok_fetch(c, turn):
            copy.wait()

        @pl.when(c + turns - 1 < chunks)
        def _():
            for copy in tok_fetch(c + turns - 1, (turn + turns - 1) % turns):
                copy.start()

        @pl.when(c + 1 < chunks)
        def _():
            fetch(c + 1).wait()

        @pl.when(c + SLOTS - 1 < chunks)
        def _():
            fetch(c + SLOTS - 1).start()

        over = score(c + 1, nxt, adds(turn, cur))

        repeats(c, turn, cur)

        @pl.when(over & (c + 1 < chunks))
        def _():
            old = m_ref[...]
            new = spread(jnp.maximum(old, peak_ref[...]))
            f = jnp.exp(old - new)
            m_ref[...] = new
            z_ref[...] = z_ref[...] * f
            pair = jnp.concatenate([f[0:1, :128], f[0:1, 128:]], axis=0)
            f96 = jnp.concatenate([pair] * 48, axis=0)

            def scale(t, carry):
                sl = pl.ds(pl.multiple_of(t * 96, 96), 96)
                hist[sl, :] = hist[sl, :] * f96
                return carry
            lax.fori_loop(0, total // 96, scale, 0)
            score(c + 1, nxt)

        @pl.when(c + 1 < chunks)
        def _():
            z_ref[...] = z_ref[...] + part_ref[...]

    for c in range(turns - 1):
        for copy in tok_fetch(c, c):
            copy.start()
    for c in range(SLOTS - 1):
        fetch(c).start()

    def clear(t, carry):
        hist[pl.ds(pl.multiple_of(t * 96, 96), 96), :] = jnp.zeros((96, 128), jnp.float32)
        return carry
    lax.fori_loop(0, total // 96, clear, 0)
    fetch(0).wait()
    m_ref[...] = jnp.zeros_like(m_ref)

    def first(t, carry):
        score(0, w_a)
        m_ref[...] = spread(peak_ref[...])
        return carry
    lax.fori_loop(0, 2, first, 0)
    z_ref[...] = part_ref[...]

    def round_of(p, carry):
        for turn in range(turns):
            cur, nxt = (w_a, w_b) if turn % 2 == 0 else (w_b, w_a)
            advance(turns * p + turn, turn, cur, nxt)
        return carry
    lax.fori_loop(0, chunks // turns, round_of, 0)

    rows = lambda v: jnp.concatenate([v[:, :128], v[:, 128:]], axis=0)
    stat_ref[0:2, :] = rows(m_ref[0:1, :])
    stat_ref[2:4, :] = rows(jnp.sum(z_ref[...], axis=0, keepdims=True))
    stat_ref[4:8, :] = jnp.zeros((4, 128), jnp.float32)
    part = total // 8
    copies = [pltpu.make_async_copy(hist.at[pl.ds(p * part, part), :], out_ref.at[pl.ds(p * part, part), :], sems.at[p])
              for p in range(8)]
    for copy in copies:
        copy.start()
    for copy in copies:
        copy.wait()


def histogram(keys, qt, tok, inv_tau, vocab):
    count, depth = keys.shape
    chunks = count // CHUNK
    stride = CHUNK // UNROLL
    members = tok.reshape(chunks, UNROLL, stride)
    ahead = jnp.concatenate([jnp.full((chunks, UNROLL, 1), -1, tok.dtype), members[:, :, :-1]], axis=2)
    again = []
    for u in range(UNROLL):
        at = members[:, u:u + 1]
        again.append(functools.reduce(
            jnp.logical_or, [members[:, o] == at[:, 0] for o in range(u)] + [ahead[:, o] == at[:, 0] for o in range(UNROLL)]))
    again = jnp.stack(again, axis=1)
    rows = 2 * members
    used = jnp.where(again, 2 * vocab, rows)
    group = jnp.where(jnp.any(again, axis=1), lax.broadcasted_iota(jnp.int32, (chunks, stride), 1), stride)
    coming = lax.cummin(group, axis=1, reverse=True)
    follow = jnp.concatenate([coming[:, 1:], jnp.full((chunks, 1), stride, jnp.int32)], axis=1)
    f32 = jnp.float32
    return pl.pallas_call(
        hist_kernel,
        out_shape=(jax.ShapeDtypeStruct((2 * vocab, 128), f32), jax.ShapeDtypeStruct((8, 128), f32)),
        in_specs=[pl.BlockSpec(memory_space=pltpu.SMEM)] * 4 + [
            pl.BlockSpec(memory_space=pl.ANY),
            pl.BlockSpec(memory_space=pl.ANY),
            pl.BlockSpec(memory_space=pl.ANY),
            pl.BlockSpec(memory_space=pltpu.VMEM),
        ],
        out_specs=(pl.BlockSpec(memory_space=pl.ANY), pl.BlockSpec(memory_space=pltpu.VMEM)),
        scratch_shapes=[
            pltpu.VMEM((2 * vocab + 8, 128), f32),
            pltpu.VMEM((2 * CHUNK, 128), f32),
            pltpu.VMEM((2 * CHUNK, 128), f32),
            pltpu.VMEM((SLOTS, CHUNK, depth), keys.dtype),
            *[pltpu.SMEM((1, CHUNK), jnp.int32)] * 4,
            pltpu.SMEM((4, 1, CHUNK), jnp.int32),
            pltpu.VMEM((8, qt.shape[1]), f32),
            pltpu.VMEM((8, qt.shape[1]), f32),
            pltpu.VMEM((8, qt.shape[1]), f32),
            pltpu.VMEM((8, qt.shape[1]), f32),
            pltpu.SemaphoreType.DMA((8,)),
            pltpu.SemaphoreType.DMA((SLOTS,)),
            pltpu.SemaphoreType.DMA((4, 2)),
        ],
        compiler_params=pltpu.CompilerParams(vmem_limit_bytes=67043328),
        name="histogram",
    )(inv_tau, jnp.zeros((1,), jnp.int32), coming[:, 0], follow.reshape(-1), used.reshape(chunks, 1, CHUNK), rows.reshape(chunks, 1, CHUNK), keys, qt)


def exchange_kernel(group, mix_ref, stat_ref, qt_ref, hist_ref, wt_ref, out_ref,
                    sib, fwd, fin, own, lm, wtile, obuf, stats, lmstat, lmstats,
                    sib_send, sib_recv, fwd_send, fwd_recv, fin_send, fin_recv,
                    st_send, st_recv, ls_send, ls_recv, own_sem, w_sem, o_sem):
    chips = group // 2
    me = lax.axis_index("model")
    x, core = me // 2, me % 2
    sibling = 2 * x + 1 - core
    right = 2 * ((x + 1) % chips) + core
    left = 2 * ((x + chips - 1) % chips) + core
    side = (right, left)
    subs = fwd.shape[1]
    rows = fwd.shape[2]
    toks = rows // 2
    half_rows = subs * rows
    block_rows = 2 * half_rows
    where = lambda d: dict(device_id={"model": d}, device_id_type=pl.DeviceIdType.MESH)

    def place(stage, s, d, c):
        chip = {0: (x + 2) % chips, 1: (x + (1, chips - 1)[d]) % chips, 2: (x + (1, chips - 1)[d]) % chips, 3: x}[stage]
        half = 1 - d if stage == 1 else d
        return pl.ds(pl.multiple_of((2 * chip + c) * block_rows + half * half_rows + s * rows, 8), rows)

    def order(stage, s, d):
        return (stage * subs + s) * 2 + d

    def to_sibling(stage, s, d):
        k = order(stage, s, d)
        return pltpu.make_async_remote_copy(hist_ref.at[place(stage, s, d, 1 - core), :], sib.at[k],
                                            sib_send.at[k], sib_recv.at[k], **where(sibling))

    def own_copy(stage, s, d):
        return pltpu.make_async_copy(hist_ref.at[place(stage, s, d, core), :], own.at[d], own_sem.at[d])

    def hop(d, s):
        return pltpu.make_async_remote_copy(sib.at[order(0, s, d)], fwd.at[d, s], fwd_send.at[d, s], fwd_recv.at[d, s], **where(side[d]))

    def last(d, stage, s):
        k = (stage - 1) * subs + s
        return pltpu.make_async_remote_copy(sib.at[order(stage, s, d)], fin.at[d, k], fin_send.at[d, k], fin_recv.at[d, k], **where(side[d]))

    barrier = pltpu.get_barrier_semaphore()
    for j in range(1, group):
        pl.semaphore_signal(barrier, inc=1, **where((me + j) % group))
    pl.semaphore_wait(barrier, group - 1)

    def stat_copy(j):
        return pltpu.make_async_remote_copy(stat_ref, stats.at[me], st_send.at[j], st_recv.at[j], **where((me + j) % group))

    for j in range(1, group):
        stat_copy(j).start()
    for stage in range(4):
        def issue(s, c, stage=stage):
            for d in range(2):
                to_sibling(stage, s, d).start()
            return c
        lax.fori_loop(0, subs, issue, 0)
    own_copy(0, 0, 0).start()
    own_copy(0, 0, 1).start()
    stats[me] = stat_ref[...]
    tiles = lm.shape[0] // toks

    def w_copy(t):
        return pltpu.make_async_copy(wt_ref.at[pl.ds(t * toks, toks), :], wtile, w_sem)
    w_copy(0).start()
    for j in range(1, group):
        stat_copy(j).wait()

    ms = [stats[i, 0:2, :] for i in range(group)]
    top = functools.reduce(jnp.maximum, ms)
    total = functools.reduce(jnp.add, [stats[i, 2:4, :] * jnp.exp(ms[i] - top) for i in range(group)])
    tile8 = lambda v: jnp.concatenate([v] * 4, axis=0)[None]
    mine = tile8(jnp.exp(stats[me, 0:2, :] - top))
    other = tile8(jnp.exp(stats[sibling, 0:2, :] - top))
    fold = lambda v: v.reshape(rows // 8, 8, 128)

    def merge(stage, s, d):
        k = order(stage, s, d)
        own_copy(stage, s, d).wait()
        to_sibling(stage, s, d).wait_recv()
        return fold(own[d]) * mine + fold(sib[k]) * other

    def prefetch(stage, s, d):
        @pl.when(s + 1 < subs)
        def _():
            own_copy(stage, s + 1, d).start()
        if stage < 3:
            @pl.when(s + 1 == subs)
            def _():
                own_copy(stage + 1, 0, d).start()

    def stage0(s, c):
        for d in range(2):
            v = merge(0, s, d)
            sib[order(0, s, d)] = v.reshape(rows, 128)
            hop(d, s).start()
            prefetch(0, s, d)
        return c
    lax.fori_loop(0, subs, stage0, 0)

    def stage1(s, c):
        for d in range(2):
            v = merge(1, s, d)
            sib[order(1, s, d)] = v.reshape(rows, 128)
            last(d, 1, s).start()
            prefetch(1, s, d)
        return c
    lax.fori_loop(0, subs, stage1, 0)

    qt = qt_ref[...]
    peak = None
    for t in range(tiles):
        w_copy(t).wait()
        logits = jnp.dot(wtile[...], qt, preferred_element_type=jnp.float32)
        lm[pl.ds(t * toks, toks), :] = logits
        if t + 1 < tiles:
            w_copy(t + 1).start()
        mx = jnp.max(logits.reshape(toks // 8, 8, 256), axis=0)
        peak = mx if peak is None else jnp.maximum(peak, mx)
    peak = jnp.max(peak, axis=0, keepdims=True)

    def expo(t, acc):
        sl = pl.ds(pl.multiple_of(t * 48, 48), 48)
        e = jnp.exp(lm[sl, :] - peak)
        lm[sl, :] = e
        return acc + jnp.sum(e.reshape(6, 8, 256), axis=0)
    acc = lax.fori_loop(0, lm.shape[0] // 48, expo, jnp.zeros((8, 256), jnp.float32))
    acc = jnp.sum(acc, axis=0, keepdims=True)
    lmstat[0:1, :] = peak
    lmstat[1:2, :] = acc
    lmstat[2:8, :] = jnp.zeros((6, 256), jnp.float32)
    lmstats[me, 0:1, :] = peak
    lmstats[me, 1:2, :] = acc

    def ls_copy(j):
        return pltpu.make_async_remote_copy(lmstat, lmstats.at[me], ls_send.at[j], ls_recv.at[j], **where((me + j) % group))

    def stage2(s, c):
        for d in range(2):
            v = merge(2, s, d)
            hop(d, s).wait_recv()
            sib[order(2, s, d)] = (v + fold(fwd[d, s])).reshape(rows, 128)
            last(d, 2, s).start()
            prefetch(2, s, d)
        return c

    for j in range(1, group):
        ls_copy(j).start()
    lax.fori_loop(0, subs, stage2, 0)
    for j in range(1, group):
        ls_copy(j).wait()

    lms = [lmstats[i, 0:1, :] for i in range(group)]
    lm_top = functools.reduce(jnp.maximum, lms)
    lm_total = functools.reduce(jnp.add, [lmstats[i, 1:2, :] * jnp.exp(lms[i] - lm_top) for i in range(group)])
    mix = mix_ref[0]
    lm_scale = (1.0 - mix) * (jnp.exp(peak - lm_top) / lm_total)
    knn_scale = mix / total
    knn_row = jnp.concatenate([knn_scale[0:1], knn_scale[1:2]], axis=1)

    def out_copy(s, d):
        return pltpu.make_async_copy(obuf.at[d], out_ref.at[pl.ds(pl.multiple_of((d * subs + s) * toks, 8), toks), :], o_sem.at[d])

    def stage3(s, c):
        for d in range(2):
            k = order(3, s, d)
            v = merge(3, s, d)
            last(1 - d, 1, s).wait_recv()
            v = v + fold(fin[1 - d, s])
            last(d, 2, s).wait_recv()
            v = v + fold(fin[d, subs + s])
            sib[k] = v.reshape(rows, 128)
            prefetch(3, s, d)

            @pl.when(s > 0)
            def _():
                out_copy(s - 1, d).wait()
            hk = jnp.concatenate([sib[k, pl.ds(0, toks, stride=2), :], sib[k, pl.ds(1, toks, stride=2), :]], axis=1)
            e = lm[pl.ds(pl.multiple_of((d * subs + s) * toks, 8), toks), :]
            obuf[d] = hk * knn_row + e * lm_scale
            out_copy(s, d).start()
        return c
    lax.fori_loop(0, subs, stage3, 0)
    for d in range(2):
        out_copy(subs - 1, d).wait()

    def drain(s, c):
        for stage in range(4):
            for d in range(2):
                to_sibling(stage, s, d).wait_send()
        for d in range(2):
            hop(d, s).wait_send()
            last(d, 1, s).wait_send()
            last(d, 2, s).wait_send()
        return c
    lax.fori_loop(0, subs, drain, 0)


def exchange(hist, stat, qt, wt, mix, group):
    cols = wt.shape[0]
    subs = next(n for n in range(3, cols) if cols % (2 * n * 8) == 0)
    toks = cols // (2 * subs)
    rows = 2 * toks
    dma = pltpu.SemaphoreType.DMA
    f32 = jnp.float32
    return pl.pallas_call(
        functools.partial(exchange_kernel, group),
        out_shape=jax.ShapeDtypeStruct((cols, qt.shape[1]), f32),
        in_specs=[
            pl.BlockSpec(memory_space=pltpu.SMEM),
            pl.BlockSpec(memory_space=pltpu.VMEM),
            pl.BlockSpec(memory_space=pltpu.VMEM),
            pl.BlockSpec(memory_space=pl.ANY),
            pl.BlockSpec(memory_space=pl.ANY),
        ],
        out_specs=pl.BlockSpec(memory_space=pl.ANY),
        scratch_shapes=[
            pltpu.VMEM((8 * subs, rows, 128), f32),
            pltpu.VMEM((2, subs, rows, 128), f32),
            pltpu.VMEM((2, 2 * subs, rows, 128), f32),
            pltpu.VMEM((2, rows, 128), f32),
            pltpu.VMEM((cols, qt.shape[1]), f32),
            pltpu.VMEM((toks, wt.shape[1]), wt.dtype),
            pltpu.VMEM((2, toks, qt.shape[1]), f32),
            pltpu.VMEM((group, 8, 128), f32),
            pltpu.VMEM((8, qt.shape[1]), f32),
            pltpu.VMEM((group, 8, qt.shape[1]), f32),
            dma((8 * subs,)), dma((8 * subs,)),
            dma((2, subs)), dma((2, subs)),
            dma((2, 2 * subs)), dma((2, 2 * subs)),
            dma((group,)), dma((group,)), dma((group,)), dma((group,)),
            dma((2,)), dma, dma((2,)),
        ],
        compiler_params=pltpu.CompilerParams(collective_id=0, has_side_effects=True, vmem_limit_bytes=67043328),
        name="exchange",
    )(mix, stat, qt, hist, wt)


def solution(mesh):
    group = mesh.shape["model"]

    def local_step(queries, w_shard, key_shard, tok_shard, temperature, mix_weight):
        qt = queries.T
        vocab = w_shard.shape[1] * group
        hist, stat = histogram(key_shard, qt, tok_shard, 1.0 / temperature, vocab)
        mixed = exchange(hist, stat, qt, w_shard.T, mix_weight, group)
        return jnp.log(mixed).T

    return jax.shard_map(
        local_step,
        mesh=mesh,
        in_specs=(P("data", None), P(None, "model"), P("model", None), P("model"), P(), P()),
        out_specs=P("data", "model"),
        check_vma=False,
    )
```
